32 devices in a mesh: wave: 2 (over x), plane: 16 (over z, y, core).
Axes of the slice: x: 2, y: 2, z: 4, core: 2. Of those that a mesh axis runs over, the one named last changes fastest.
Arguments:
- right_side: float32 [2, 128, 128], P('wave', 'plane'), may hold values from -40 to 40
- coupling_x: float32 [128, 128], P('plane'), may hold values from 2 to 6
- coupling_y: float32 [2, 128], P('wave'), may hold values from 0.2 to 0.6
- coupling_z: float32 [2, 128, 128], P('wave', 'plane'), may hold values from 0.3 to 1
- inverse: float32 [2, 128, 128, 128], P('wave', 'plane'), may hold values from -0.05 to 0.15
Outputs:
- solution: float32 [2, 128, 128], P('wave', 'plane')
- residual: float32 [2, 128, 128], P('wave', 'plane')
The draws below stay inside these ranges and needn't reach their ends.
All inputs are finite; a program needn't handle non-finite values.
Results may differ from the reference program's by a relative error of at most 0.0003.
Values sent between devices are 32-bit elements; how exact they have to be, the bound alone decides.
A program may use at most 64 MiB of HBM per device.

```python
import math
import jax
import jax.numpy as jnp
from jax import lax

B = 128
ITERS = 2
NX = 2
NY = 128


def draw_right_side(key, part):
    first = jax.random.fold_in(jax.random.fold_in(key, 11), 0)
    xs = jnp.arange(NX, dtype=jnp.float32)[:, None, None] / NX
    ys = jnp.arange(NY, dtype=jnp.float32)[None, :, None] / NY
    ramp = jnp.power(3.0, ys) * jnp.power(3.0, xs)
    return jnp.clip(jax.random.normal(first, (NX, NY, B), jnp.float32), -4.0, 4.0) * ramp


def draw_inverse(key, part):
    first, second = jax.random.split(jax.random.fold_in(key, 23))
    diagonal = jax.random.uniform(first, (NX, NY, B), jnp.float32, 0.08, 0.13)
    spread = 0.025
    noise = jax.random.normal(second, (NX, NY, B, B), jnp.float32)
    symmetric = (noise + jnp.swapaxes(noise, -1, -2)) * (spread / (1.4142135 * jnp.sqrt(jnp.float32(B))))
    identity = jnp.eye(B, dtype=jnp.float32)
    return symmetric * (1.0 - identity) + diagonal[..., None] * identity


def block_scale(key, shape, cuts, least, high):
    def one(position, shards_of):
        heights = jax.random.uniform(jax.random.fold_in(jax.random.fold_in(key, 6), position), (shards_of,), jnp.float32, least / len(cuts), high / len(cuts))
        return jnp.repeat(jnp.exp(heights), shape[position] // shards_of).reshape((-1,) + (1,) * (len(shape) - position - 1))

    loudness = one(*cuts[0])
    for cut in cuts[1:]:
        loudness = loudness * one(*cut)
    return loudness


def setup_inputs(seed: int = 0) -> dict:
    key_of = jax.random.split(jax.random.key(seed), 6)
    return {
        "right_side": draw_right_side(jax.random.fold_in(key_of[5], 71), 0),
        "coupling_x": jnp.clip(jnp.exp(math.log(6.0) - 1.0986123 * jax.random.uniform(key_of[1], (NY, B), jnp.float32) ** block_scale(key_of[1], (NY, B), ((0, 16),), -0.2, 0.2)), 2.0, 6.0),
        "coupling_y": jnp.clip(jnp.exp(math.log(0.6) - 1.0986123 * jax.random.uniform(key_of[2], (NX, B), jnp.float32) ** block_scale(key_of[2], (NX, B), ((0, 2),), -0.2, 0.2)), 0.2, 0.6),
        "coupling_z": jnp.clip(jnp.exp(math.log(1.0) - 1.2039728 * jax.random.uniform(key_of[3], (NX, NY, B), jnp.float32) ** block_scale(key_of[3], (NX, NY, B), ((0, 2), (1, 16)), -0.2, 0.2)), 0.3, 1.0),
        "inverse": draw_inverse(jax.random.fold_in(key_of[5], 71), 0),
    }


relax = 1.5


def apply_block(block, vector):
    return jnp.einsum("cij,cj->ci", block, vector, precision=lax.Precision.HIGHEST)


def column_part(values, coupling_x, coupling_y, coupling_z):
    below = jnp.concatenate([jnp.zeros_like(values[..., :1]), values[..., :-1]], axis=-1)
    above = jnp.concatenate([values[..., 1:], jnp.zeros_like(values[..., :1])], axis=-1)
    upper_z = jnp.concatenate([coupling_z[..., 1:], coupling_z[..., :1]], axis=-1)
    centre = 2.0 * coupling_x[None] + 2.0 * coupling_y[:, None] + coupling_z + upper_z
    return centre * values - coupling_z * below - upper_z * above


def operate(values, coupling_x, coupling_y, coupling_z):
    padded = jnp.pad(values, ((1, 1), (1, 1), (0, 0)))
    along_x = padded[:-2, 1:-1] + padded[2:, 1:-1]
    along_y = padded[1:-1, :-2] + padded[1:-1, 2:]
    return column_part(values, coupling_x, coupling_y, coupling_z) - coupling_x[None] * along_x - coupling_y[:, None] * along_y


def precondition(residual, inverse, coupling_x, coupling_y, coupling_z):
    def forward_step(previous, items):
        source, block = items
        fresh = relax * apply_block(block, source + coupling_x * previous)
        return fresh, fresh

    start = jnp.zeros(residual.shape[1:], jnp.float32)
    unused, half_sweep = lax.scan(forward_step, start, (residual, inverse))
    padded = jnp.pad(half_sweep, ((1, 1), (1, 1), (0, 0)))
    settled = column_part(half_sweep, coupling_x, coupling_y, coupling_z) - coupling_x[None] * padded[:-2, 1:-1]
    settled = settled - coupling_y[:, None] * (padded[1:-1, :-2] + padded[1:-1, 2:])

    def backward_step(previous, items):
        source, block, base = items
        fresh = base + relax * apply_block(block, source + coupling_x * previous)
        return fresh, fresh

    unused, result = lax.scan(backward_step, start, (residual - settled, inverse, half_sweep), reverse=True)
    return result


def reference(right_side, coupling_x, coupling_y, coupling_z, inverse):
    solution = jnp.zeros_like(right_side)
    residual = right_side
    direction = right_side
    image = right_side
    curvature = jnp.float32(1.0)
    for iteration in range(ITERS):
        precond = precondition(residual, inverse, coupling_x, coupling_y, coupling_z)
        if iteration == 0:
            direction = precond
        else:
            ratio = -jnp.sum(precond * image) / curvature
            direction = precond + ratio * direction
        image = operate(direction, coupling_x, coupling_y, coupling_z)
        projection = jnp.sum(direction * residual)
        curvature = jnp.sum(direction * image)
        step_size = projection / curvature
        solution = solution + step_size * direction
        residual = residual - step_size * image
    return solution, residual
```

```python
import functools

import jax
import jax.numpy as jnp
from jax import lax
from jax.experimental import pallas as pl
from jax.experimental.pallas import tpu as pltpu
from jax.sharding import PartitionSpec as P

relax = 1.5
MESH = pl.DeviceIdType.MESH
DIRECT = 64


def kernel(
    sections, strips,
    right_ref, cx_ref, cy_ref, cz_ref, inverse_ref,
    solution_ref, residual_ref,
    block, weights, half, field, half_edge, field_edge,
    from_lower_half, from_upper, from_lower, half_halo, field_halo,
    sums, gathered,
    load_sem, send_x, recv_x, send_y, recv_y, send_sum, recv_sum,
):
    depth, columns, cells = right_ref.shape
    w = lax.axis_index("wave")
    p = lax.axis_index("plane")
    devices = sections * strips

    load = pltpu.make_async_copy(inverse_ref, block, load_sem)
    load.start()

    barrier = pltpu.get_barrier_semaphore()
    single = devices <= DIRECT
    if single:
        groups = [(devices, w * strips + p, lambda t: (t // strips, t % strips))]
    else:
        groups = [(sections, w, lambda t: (t, p)), (strips, p, lambda t: (w, t))]
    greeted = 0
    for count, me, where in groups:
        for offset in range(1, count):
            pl.semaphore_signal(
                barrier, inc=1, device_id=where((me + offset) % count), device_id_type=MESH
            )
        greeted += count - 1

    lane = lax.broadcasted_iota(jnp.int32, (columns, cells), 1)
    row = lax.broadcasted_iota(jnp.int32, (columns, cells), 0)
    cx = cx_ref[...]
    cy, lower_z, upper_z, centre = [], [], [], []
    for d in range(depth):
        cz = cz_ref[d]
        above = pltpu.roll(cz, cells - 1, 1)
        cy.append(jnp.broadcast_to(cy_ref[d : d + 1, :], (columns, cells)))
        centre.append(2.0 * cx + 2.0 * cy[d] + cz + above)
        lower_z.append(jnp.where(lane == 0, 0.0, cz))
        upper_z.append(jnp.where(lane == cells - 1, 0.0, above))

    nothing = jnp.zeros((columns, cells), jnp.float32)
    no_edge = jnp.zeros((depth, 1, cells), jnp.float32)

    @pl.when(w == 0)
    def _():
        for k in range(2):
            from_lower_half[k] = nothing
            from_lower[k] = nothing

    @pl.when(w == sections - 1)
    def _():
        for k in range(2):
            from_upper[k] = nothing

    @pl.when(p == 0)
    def _():
        for k in range(2):
            half_halo[k, 0] = no_edge
            field_halo[k, 0] = no_edge

    @pl.when(p == strips - 1)
    def _():
        for k in range(2):
            half_halo[k, 1] = no_edge
            field_halo[k, 1] = no_edge

    load.wait()
    for d in range(depth):
        for c in range(columns):
            weights[d, pl.ds(c, cells, stride=columns), :] = block[d, c].T

    def apply_block(d, v):
        parts = [None] * 4
        for j in range(cells):
            term = weights[d, pl.ds(j * columns, columns), :] * jnp.broadcast_to(
                v[:, j : j + 1], (columns, cells)
            )
            parts[j % 4] = term if parts[j % 4] is None else parts[j % 4] + term
        return relax * ((parts[0] + parts[1]) + (parts[2] + parts[3]))

    def column_part(d, v):
        return (
            centre[d] * v
            - lower_z[d] * pltpu.roll(v, 1, 1)
            - upper_z[d] * pltpu.roll(v, cells - 1, 1)
        )

    def along_y(v, low, high):
        below = jnp.where(row == 0, low, pltpu.roll(v, 1, 0))
        above = jnp.where(row == columns - 1, high, pltpu.roll(v, columns - 1, 0))
        return below + above

    def x_copy(source, target, slot, step):
        return pltpu.make_async_remote_copy(
            src_ref=source, dst_ref=target, send_sem=send_x.at[slot], recv_sem=recv_x.at[slot],
            device_id=(w + step, p), device_id_type=MESH,
        )

    def y_copy(edges, halo, k, side, slot):
        return pltpu.make_async_remote_copy(
            src_ref=edges.at[k, side], dst_ref=halo.at[k, 1 - side],
            send_sem=send_y.at[slot + side], recv_sem=recv_y.at[slot + side],
            device_id=(w, p + (2 * side - 1)), device_id_type=MESH,
        )

    def send_edges(planes, edges, halo, k, slot):
        for d in range(depth):
            edges[k, 0, d] = planes[d][:1]
            edges[k, 1, d] = planes[d][columns - 1 :]

        @pl.when(p > 0)
        def _():
            y_copy(edges, halo, k, 0, slot).start()

        @pl.when(p < strips - 1)
        def _():
            y_copy(edges, halo, k, 1, slot).start()

    def wait_edges(edges, halo, k, slot):
        @pl.when(p > 0)
        def _():
            y_copy(edges, halo, k, 1, slot).wait_recv()

        @pl.when(p < strips - 1)
        def _():
            y_copy(edges, halo, k, 0, slot).wait_recv()

    def wait_sent(edges, halo, k, slot):
        @pl.when(p > 0)
        def _():
            y_copy(edges, halo, k, 0, slot).wait_send()

        @pl.when(p < strips - 1)
        def _():
            y_copy(edges, halo, k, 1, slot).wait_send()

    def precondition(source, k, first):
        slot = 3 * k
        edge_slot = 4 * k
        up_half = x_copy(half.at[k, depth - 1], from_lower_half.at[k], slot, 1)
        down_field = x_copy(field.at[k, 0], from_upper.at[k], slot + 1, -1)
        up_field = x_copy(field.at[k, depth - 1], from_lower.at[k], slot + 2, 1)

        if first:
            pl.semaphore_wait(barrier, greeted)

        @pl.when(w > 0)
        def _():
            up_half.wait_recv()

        lower = [from_lower_half[k]]
        h = []
        for d in range(depth):
            h.append(apply_block(d, source[d] + cx * lower[d]))
            lower.append(h[d])
            half[k, d] = h[d]

        @pl.when(w < sections - 1)
        def _():
            up_half.start()

        send_edges(h, half_edge, half_halo, k, edge_slot)
        partial = [source[d] - (column_part(d, h[d]) - cx * lower[d]) for d in range(depth)]
        wait_edges(half_edge, half_halo, k, edge_slot)
        rest = [
            partial[d] + cy[d] * along_y(h[d], half_halo[k, 0, d], half_halo[k, 1, d])
            for d in range(depth)
        ]

        @pl.when(w < sections - 1)
        def _():
            down_field.wait_recv()

        upper = from_upper[k]
        z = [None] * depth
        above = [None] * depth
        previous = upper
        for d in reversed(range(depth)):
            above[d] = previous
            z[d] = h[d] + apply_block(d, rest[d] + cx * previous)
            previous = z[d]
            field[k, d] = z[d]

        @pl.when(w > 0)
        def _():
            down_field.start()

        @pl.when(w < sections - 1)
        def _():
            up_field.start()

        send_edges(z, field_edge, field_halo, k, edge_slot + 2)
        partial = [column_part(d, z[d]) for d in range(depth)]
        wait_edges(field_edge, field_halo, k, edge_slot + 2)

        @pl.when(w > 0)
        def _():
            up_field.wait_recv()

        below = from_lower[k]
        image = []
        for d in range(depth):
            image.append(
                partial[d]
                - cx * (below + above[d])
                - cy[d] * along_y(z[d], field_halo[k, 0, d], field_halo[k, 1, d])
            )
            below = z[d]
        return z, image

    def finish(k):
        slot = 3 * k
        edge_slot = 4 * k

        @pl.when(w < sections - 1)
        def _():
            x_copy(half.at[k, depth - 1], from_lower_half.at[k], slot, 1).wait_send()
            x_copy(field.at[k, depth - 1], from_lower.at[k], slot + 2, 1).wait_send()

        @pl.when(w > 0)
        def _():
            x_copy(field.at[k, 0], from_upper.at[k], slot + 1, -1).wait_send()

        wait_sent(half_edge, half_halo, k, edge_slot)
        wait_sent(field_edge, field_halo, k, edge_slot + 2)

    right = [right_ref[d] for d in range(depth)]
    z, q = precondition(right, 0, True)
    y, u = precondition(q, 1, False)

    def inner(a, b):
        total = a[0] * b[0]
        for d in range(1, depth):
            total = total + a[d] * b[d]
        return jnp.sum(jnp.sum(total, axis=0, keepdims=True), axis=1, keepdims=True)

    spot = lax.broadcasted_iota(jnp.int32, (1, cells), 1)
    packed = jnp.zeros((1, cells), jnp.float32)
    pairs = [(z, right), (z, q), (y, q), (y, right), (y, u), (z, u)]
    for i, (a, b) in enumerate(pairs):
        packed = jnp.where(spot == i, inner(a, b), packed)

    base = 0
    for stage, (count, me, where) in enumerate(groups):
        sums[stage] = packed
        gathered[base + me] = packed

        def send(offset):
            return pltpu.make_async_remote_copy(
                src_ref=sums.at[stage], dst_ref=gathered.at[base + me],
                send_sem=send_sum.at[base + offset], recv_sem=recv_sum.at[base + me],
                device_id=where((me + offset) % count), device_id_type=MESH,
            )

        def arrival(sender):
            return pltpu.make_async_remote_copy(
                src_ref=sums.at[stage], dst_ref=gathered.at[base + sender],
                send_sem=send_sum.at[base], recv_sem=recv_sum.at[base + sender],
                device_id=where(sender), device_id_type=MESH,
            )

        for offset in range(1, count):
            send(offset).start()
        if stage == 0:
            finish(0)
            finish(1)
        for offset in range(1, count):
            arrival((me + offset) % count).wait_recv()
        parts = [gathered[base + i] for i in range(count)]
        while len(parts) > 1:
            parts = [
                parts[i] + parts[i + 1] if i + 1 < len(parts) else parts[i]
                for i in range(0, len(parts), 2)
            ]
        packed = parts[0]
        for offset in range(1, count):
            send(offset).wait_send()
        base += count

    zr, zq, yq, yr, yu, zu = [
        jnp.broadcast_to(packed[:, i : i + 1], (1, cells)) for i in range(len(pairs))
    ]
    first_step = zr / zq
    keep = 1.0 - (zq - first_step * yq) / zq
    projection = keep * (zr - first_step * zq) - first_step * (yr - first_step * yq)
    curvature = (
        keep * keep * zq - keep * first_step * (yq + zu) + first_step * first_step * yu
    )
    step = projection / curvature
    of_z = first_step + step * keep
    of_y = step * first_step
    for d in range(depth):
        solution_ref[d] = of_z * z[d] - of_y * y[d]
        residual_ref[d] = right[d] - of_z * q[d] + of_y * u[d]


def solution(mesh):
    sections = mesh.shape["wave"]
    strips = mesh.shape["plane"]

    def on_device(right_side, coupling_x, coupling_y, coupling_z, inverse):
        depth, columns, cells = right_side.shape
        devices = sections * strips
        slots = devices if devices <= DIRECT else sections + strips
        vmem = pl.BlockSpec(memory_space=pltpu.VMEM)
        plane = (columns, cells)
        out = jax.ShapeDtypeStruct(right_side.shape, jnp.float32)
        return pl.pallas_call(
            functools.partial(kernel, sections, strips),
            out_shape=(out, out),
            in_specs=[vmem] * 4 + [pl.BlockSpec(memory_space=pl.ANY)],
            out_specs=(vmem, vmem),
            scratch_shapes=[
                pltpu.VMEM(inverse.shape, jnp.float32),
                pltpu.VMEM((depth, cells * columns, cells), jnp.float32),
                pltpu.VMEM((2, depth) + plane, jnp.float32),
                pltpu.VMEM((2, depth) + plane, jnp.float32),
                pltpu.VMEM((2, 2, depth, 1, cells), jnp.float32),
                pltpu.VMEM((2, 2, depth, 1, cells), jnp.float32),
                pltpu.VMEM((2,) + plane, jnp.float32),
                pltpu.VMEM((2,) + plane, jnp.float32),
                pltpu.VMEM((2,) + plane, jnp.float32),
                pltpu.VMEM((2, 2, depth, 1, cells), jnp.float32),
                pltpu.VMEM((2, 2, depth, 1, cells), jnp.float32),
                pltpu.VMEM((2, 1, cells), jnp.float32),
                pltpu.VMEM((slots, 1, cells), jnp.float32),
                pltpu.SemaphoreType.DMA,
                pltpu.SemaphoreType.DMA((6,)),
                pltpu.SemaphoreType.DMA((6,)),
                pltpu.SemaphoreType.DMA((8,)),
                pltpu.SemaphoreType.DMA((8,)),
                pltpu.SemaphoreType.DMA((slots,)),
                pltpu.SemaphoreType.DMA((slots,)),
            ],
            compiler_params=pltpu.CompilerParams(collective_id=0, has_side_effects=True),
        )(right_side, coupling_x, coupling_y, coupling_z, inverse)

    placed = (
        P("wave", "plane", None),
        P("plane", None),
        P("wave", None),
        P("wave", "plane", None),
        P("wave", "plane", None, None),
    )
    return jax.shard_map(
        on_device,
        mesh=mesh,
        in_specs=placed,
        out_specs=(P("wave", "plane", None), P("wave", "plane", None)),
        check_vma=False,
    )
```

```python
import functools

import jax
import jax.numpy as jnp
from jax import lax
from jax.experimental import pallas as pl
from jax.experimental.pallas import tpu as pltpu
from jax.sharding import PartitionSpec as P

relax = 1.5
MESH = pl.DeviceIdType.MESH
DIRECT = 64


def kernel(
    sections, strips,
    right_any, cx_any, cy_any, cz_any, inverse_any,
    solution_ref, residual_ref,
    right_ref, cx_ref, cy_ref, cz_ref, block, weights, half, field, half_edge, field_edge,
    from_lower_half, from_upper, from_lower, half_halo, field_halo,
    sums, gathered,
    load_sem, send_x, recv_x, send_y, recv_y, send_sum, recv_sum,
):
    depth, columns, cells = right_ref.shape
    w = lax.axis_index("wave")
    p = lax.axis_index("plane")
    devices = sections * strips

    barrier = pltpu.get_barrier_semaphore()
    single = devices <= DIRECT
    if single:
        groups = [(devices, w * strips + p, lambda t: (t // strips, t % strips))]
    else:
        groups = [(strips, p, lambda t: (w, t)), (sections, w, lambda t: (t, p))]
    greeted = 0
    for count, me, where in groups:
        for offset in range(1, count):
            pl.semaphore_signal(
                barrier, inc=1, device_id=where((me + offset) % count), device_id_type=MESH
            )
        greeted += count - 1

    loads = [
        pltpu.make_async_copy(source, target, load_sem.at[i])
        for i, (source, target) in enumerate(
            [
                (inverse_any, block), (cz_any, cz_ref), (cx_any, cx_ref),
                (cy_any, cy_ref), (right_any, right_ref),
            ]
        )
    ]
    for load in loads:
        load.start()
    for load in loads[1:]:
        load.wait()

    lane = lax.broadcasted_iota(jnp.int32, (columns, cells), 1)
    row = lax.broadcasted_iota(jnp.int32, (columns, cells), 0)
    cx = cx_ref[...]
    cy, lower_z, upper_z, centre = [], [], [], []
    for d in range(depth):
        cz = cz_ref[d]
        above = pltpu.roll(cz, cells - 1, 1)
        cy.append(jnp.broadcast_to(cy_ref[d : d + 1, :], (columns, cells)))
        centre.append(2.0 * cx + 2.0 * cy[d] + cz + above)
        lower_z.append(jnp.where(lane == 0, 0.0, cz))
        upper_z.append(jnp.where(lane == cells - 1, 0.0, above))

    nothing = jnp.zeros((columns, cells), jnp.float32)
    no_edge = jnp.zeros((depth, 1, cells), jnp.float32)

    @pl.when(w == 0)
    def _():
        for k in range(2):
            from_lower_half[k] = nothing
            from_lower[k] = nothing

    @pl.when(w == sections - 1)
    def _():
        for k in range(2):
            from_upper[k] = nothing

    @pl.when(p == 0)
    def _():
        for k in range(2):
            half_halo[k, 0] = no_edge
            field_halo[k, 0] = no_edge

    @pl.when(p == strips - 1)
    def _():
        for k in range(2):
            half_halo[k, 1] = no_edge
            field_halo[k, 1] = no_edge

    loads[0].wait()
    for d in range(depth):
        for c in range(columns):
            weights[d, pl.ds(c, cells, stride=columns), :] = block[d, c].T

    def apply_block(d, v):
        parts = [None] * 4
        for j in range(cells):
            term = weights[d, pl.ds(j * columns, columns), :] * jnp.broadcast_to(
                v[:, j : j + 1], (columns, cells)
            )
            parts[j % 4] = term if parts[j % 4] is None else parts[j % 4] + term
        return relax * ((parts[0] + parts[1]) + (parts[2] + parts[3]))

    def column_part(d, v):
        return (
            centre[d] * v
            - lower_z[d] * pltpu.roll(v, 1, 1)
            - upper_z[d] * pltpu.roll(v, cells - 1, 1)
        )

    def along_y(v, low, high):
        below = jnp.where(row == 0, low, pltpu.roll(v, 1, 0))
        above = jnp.where(row == columns - 1, high, pltpu.roll(v, columns - 1, 0))
        return below + above

    def x_copy(source, target, slot, step):
        return pltpu.make_async_remote_copy(
            src_ref=source, dst_ref=target, send_sem=send_x.at[slot], recv_sem=recv_x.at[slot],
            device_id=(w + step, p), device_id_type=MESH,
        )

    def y_copy(edges, halo, k, side, slot):
        return pltpu.make_async_remote_copy(
            src_ref=edges.at[k, side], dst_ref=halo.at[k, 1 - side],
            send_sem=send_y.at[slot + side], recv_sem=recv_y.at[slot + side],
            device_id=(w, p + (2 * side - 1)), device_id_type=MESH,
        )

    def send_edges(planes, edges, halo, k, slot):
        for d in range(depth):
            edges[k, 0, d] = planes[d][:1]
            edges[k, 1, d] = planes[d][columns - 1 :]

        @pl.when(p > 0)
        def _():
            y_copy(edges, halo, k, 0, slot).start()

        @pl.when(p < strips - 1)
        def _():
            y_copy(edges, halo, k, 1, slot).start()

    def wait_edges(edges, halo, k, slot):
        @pl.when(p > 0)
        def _():
            y_copy(edges, halo, k, 1, slot).wait_recv()

        @pl.when(p < strips - 1)
        def _():
            y_copy(edges, halo, k, 0, slot).wait_recv()

    def wait_sent(edges, halo, k, slot):
        @pl.when(p > 0)
        def _():
            y_copy(edges, halo, k, 0, slot).wait_send()

        @pl.when(p < strips - 1)
        def _():
            y_copy(edges, halo, k, 1, slot).wait_send()

    def precondition(source, k, meanwhile):
        slot = 3 * k
        edge_slot = 4 * k
        up_half = x_copy(half.at[k, depth - 1], from_lower_half.at[k], slot, 1)
        down_field = x_copy(field.at[k, 0], from_upper.at[k], slot + 1, -1)
        up_field = x_copy(field.at[k, depth - 1], from_lower.at[k], slot + 2, 1)

        @pl.when(w > 0)
        def _():
            up_half.wait_recv()

        lower = [from_lower_half[k]]
        h = []
        for d in range(depth):
            h.append(apply_block(d, source[d] + cx * lower[d]))
            lower.append(h[d])
            half[k, d] = h[d]

        if k == 0:
            pl.semaphore_wait(barrier, greeted)

        @pl.when(w < sections - 1)
        def _():
            up_half.start()

        send_edges(h, half_edge, half_halo, k, edge_slot)
        meanwhile()
        partial = [source[d] - (column_part(d, h[d]) - cx * lower[d]) for d in range(depth)]
        wait_edges(half_edge, half_halo, k, edge_slot)
        rest = [
            partial[d] + cy[d] * along_y(h[d], half_halo[k, 0, d], half_halo[k, 1, d])
            for d in range(depth)
        ]

        @pl.when(w < sections - 1)
        def _():
            down_field.wait_recv()

        upper = from_upper[k]
        z = [None] * depth
        above = [None] * depth
        previous = upper
        for d in reversed(range(depth)):
            above[d] = previous
            z[d] = h[d] + apply_block(d, rest[d] + cx * previous)
            previous = z[d]
            field[k, d] = z[d]

        @pl.when(w > 0)
        def _():
            down_field.start()

        @pl.when(w < sections - 1)
        def _():
            up_field.start()

        send_edges(z, field_edge, field_halo, k, edge_slot + 2)
        return z, above, [column_part(d, z[d]) for d in range(depth)]

    def operate(k, z, above, partial):
        edge_slot = 4 * k
        wait_edges(field_edge, field_halo, k, edge_slot + 2)

        @pl.when(w > 0)
        def _():
            x_copy(field.at[k, depth - 1], from_lower.at[k], 3 * k + 2, 1).wait_recv()

        below = from_lower[k]
        image = []
        for d in range(depth):
            image.append(
                partial[d]
                - cx * (below + above[d])
                - cy[d] * along_y(z[d], field_halo[k, 0, d], field_halo[k, 1, d])
            )
            below = z[d]
        return image

    def finish(k):
        slot = 3 * k
        edge_slot = 4 * k

        @pl.when(w < sections - 1)
        def _():
            x_copy(half.at[k, depth - 1], from_lower_half.at[k], slot, 1).wait_send()
            x_copy(field.at[k, depth - 1], from_lower.at[k], slot + 2, 1).wait_send()

        @pl.when(w > 0)
        def _():
            x_copy(field.at[k, 0], from_upper.at[k], slot + 1, -1).wait_send()

        wait_sent(half_edge, half_halo, k, edge_slot)
        wait_sent(field_edge, field_halo, k, edge_slot + 2)

    def inner(a, b):
        total = a[0] * b[0]
        for d in range(1, depth):
            total = total + a[d] * b[d]
        return jnp.sum(jnp.sum(total, axis=0, keepdims=True), axis=1, keepdims=True)

    spot = lax.broadcasted_iota(jnp.int32, (1, cells), 1)
    rows = 1 + 2 * depth
    right = [right_ref[d] for d in range(depth)]
    z, above, partial = precondition(right, 0, lambda: None)
    q = operate(0, z, above, partial)

    def early():
        sums[0, 0] = jnp.where(
            spot == 0, inner(z, right), jnp.where(spot == 1, inner(z, q), 0.0)
        )

    y, above, partial = precondition(q, 1, early)
    faced = []
    for d in range(depth):
        next_column = jnp.where(row == columns - 1, 0.0, pltpu.roll(y[d], columns - 1, 0))
        faced.append(partial[d] - 2.0 * (cx * above[d] + cy[d] * next_column))
        sums[0, 1 + 2 * d] = y[d][:1]
        sums[0, 2 + 2 * d] = cy[d][:1] * y[d][columns - 1 :]
    packed = sums[0, 0]
    for i, (a, b) in enumerate([(y, q), (y, right), (y, faced)]):
        packed = jnp.where(spot == 2 + i, inner(a, b), packed)

    base = 0
    for stage, (count, me, where) in enumerate(groups):
        width = rows if stage == 0 else 1
        sums[stage, 0] = packed

        def send(offset):
            return pltpu.make_async_remote_copy(
                src_ref=sums.at[stage, pl.ds(0, width)],
                dst_ref=gathered.at[base + me, pl.ds(0, width)],
                send_sem=send_sum.at[base + offset], recv_sem=recv_sum.at[base + me],
                device_id=where((me + offset) % count), device_id_type=MESH,
            )

        def arrival(sender):
            return pltpu.make_async_remote_copy(
                src_ref=sums.at[stage, pl.ds(0, width)],
                dst_ref=gathered.at[base + sender, pl.ds(0, width)],
                send_sem=send_sum.at[base], recv_sem=recv_sum.at[base + sender],
                device_id=where(sender), device_id_type=MESH,
            )

        for offset in range(1, count):
            send(offset).start()
        for i in range(width):
            gathered[base + me, i] = sums[stage, i]
        if stage == 0:
            u = operate(1, y, above, partial)
            finish(0)
            finish(1)
        for offset in range(1, count):
            arrival((me + offset) % count).wait_recv()

        def tree(parts):
            while len(parts) > 1:
                parts = [
                    parts[i] + parts[i + 1] if i + 1 < len(parts) else parts[i]
                    for i in range(0, len(parts), 2)
                ]
            return parts[0]

        packed = tree([gathered[base + i, 0] for i in range(count)])
        faces = [
            gathered[base + i, 2 + 2 * d] * gathered[base + i + 1, 1 + 2 * d]
            for i in range(count)
            if stage == 0 and i % strips != strips - 1
            for d in range(depth)
        ]
        if faces:
            across = jnp.sum(tree(faces), axis=1, keepdims=True)
            packed = jnp.where(spot == 4, packed - 2.0 * across, packed)
        for offset in range(1, count):
            send(offset).wait_send()
        base += count

    zr, zq, yq, yr, yu = [
        jnp.broadcast_to(packed[:, i : i + 1], (1, cells)) for i in range(5)
    ]
    first_step = zr / zq
    keep = 1.0 - (zq - first_step * yq) / zq
    projection = keep * (zr - first_step * zq) - first_step * (yr - first_step * yq)
    curvature = (
        keep * keep * zq - keep * 2.0 * first_step * yq + first_step * first_step * yu
    )
    step = projection / curvature
    of_z = first_step + step * keep
    of_y = step * first_step
    for d in range(depth):
        solution_ref[d] = of_z * z[d] - of_y * y[d]
        residual_ref[d] = right[d] - of_z * q[d] + of_y * u[d]


def solution(mesh):
    sections = mesh.shape["wave"]
    strips = mesh.shape["plane"]

    def on_device(right_side, coupling_x, coupling_y, coupling_z, inverse):
        depth, columns, cells = right_side.shape
        devices = sections * strips
        slots = devices if devices <= DIRECT else sections + strips
        vmem = pl.BlockSpec(memory_space=pltpu.VMEM)
        plane = (columns, cells)
        out = pltpu.VMEM(right_side.shape, jnp.float32)
        rows = 1 + 2 * depth
        return pl.pallas_call(
            functools.partial(kernel, sections, strips),
            out_shape=(out, out),
            in_specs=[pl.BlockSpec(memory_space=pl.ANY)] * 5,
            out_specs=(vmem, vmem),
            scratch_shapes=[
                pltpu.VMEM(right_side.shape, jnp.float32),
                pltpu.VMEM(coupling_x.shape, jnp.float32),
                pltpu.VMEM(coupling_y.shape, jnp.float32),
                pltpu.VMEM(coupling_z.shape, jnp.float32),
                pltpu.VMEM(inverse.shape, jnp.float32),
                pltpu.VMEM((depth, cells * columns, cells), jnp.float32),
                pltpu.VMEM((2, depth) + plane, jnp.float32),
                pltpu.VMEM((2, depth) + plane, jnp.float32),
                pltpu.VMEM((2, 2, depth, 1, cells), jnp.float32),
                pltpu.VMEM((2, 2, depth, 1, cells), jnp.float32),
                pltpu.VMEM((2,) + plane, jnp.float32),
                pltpu.VMEM((2,) + plane, jnp.float32),
                pltpu.VMEM((2,) + plane, jnp.float32),
                pltpu.VMEM((2, 2, depth, 1, cells), jnp.float32),
                pltpu.VMEM((2, 2, depth, 1, cells), jnp.float32),
                pltpu.VMEM((2, rows, 1, cells), jnp.float32),
                pltpu.VMEM((slots, rows, 1, cells), jnp.float32),
                pltpu.SemaphoreType.DMA((5,)),
                pltpu.SemaphoreType.DMA((6,)),
                pltpu.SemaphoreType.DMA((6,)),
                pltpu.SemaphoreType.DMA((8,)),
                pltpu.SemaphoreType.DMA((8,)),
                pltpu.SemaphoreType.DMA((slots,)),
                pltpu.SemaphoreType.DMA((slots,)),
            ],
            compiler_params=pltpu.CompilerParams(collective_id=0, has_side_effects=True),
        )(right_side, coupling_x, coupling_y, coupling_z, inverse)

    placed = (
        P("wave", "plane", None),
        P("plane", None),
        P("wave", None),
        P("wave", "plane", None),
        P("wave", "plane", None, None),
    )
    return jax.shard_map(
        on_device,
        mesh=mesh,
        in_specs=placed,
        out_specs=(P("wave", "plane", None), P("wave", "plane", None)),
        check_vma=False,
    )
```

```python
import functools

import jax
import jax.numpy as jnp
from jax import lax
from jax.experimental import pallas as pl
from jax.experimental.pallas import tpu as pltpu
from jax.sharding import PartitionSpec as P

relax = 1.5
MESH = pl.DeviceIdType.MESH
DIRECT = 64
RIM_FIRST = False


def kernel(
    sections, strips,
    right_any, cx_any, cy_any, cz_any, inverse_any,
    solution_ref, residual_ref,
    right_ref, cx_ref, cy_ref, cz_ref, block, weights, half, field, half_edge, field_edge,
    from_lower_half, from_upper, from_lower, half_halo, field_halo,
    still_edge, still_rim, block_rim, weights_rim, half_rim, field_rim,
    lower_half_rim, upper_field_rim, lower_field_rim,
    sums, gathered,
    load_sem, send_x, recv_x, send_y, recv_y, send_d, recv_d, send_still, recv_still, send_sum, recv_sum,
):
    depth, columns, cells = right_ref.shape
    w = lax.axis_index("wave")
    p = lax.axis_index("plane")
    devices = sections * strips

    barrier = pltpu.get_barrier_semaphore()
    single = devices <= DIRECT
    if single:
        groups = [(devices, w * strips + p, lambda t: (t // strips, t % strips))]
    else:
        groups = [(strips, p, lambda t: (w, t)), (sections, w, lambda t: (t, p))]
    greeted = 0
    for count, me, where in groups:
        for offset in range(1, count):
            pl.semaphore_signal(
                barrier, inc=1, device_id=where((me + offset) % count), device_id_type=MESH
            )
        greeted += count - 1
    if not single:
        for a in (-1, 1):
            for b in (-1, 1):
                near = (
                    (w + a >= 0) & (w + a < sections) & (p + b >= 0) & (p + b < strips)
                )
                greeted = greeted + near.astype(jnp.int32)

                @pl.when(near)
                def _():
                    pl.semaphore_signal(
                        barrier, inc=1, device_id=(w + a, p + b), device_id_type=MESH
                    )

    loads = [
        pltpu.make_async_copy(source, target, load_sem.at[i])
        for i, (source, target) in enumerate(
            [
                (inverse_any, block), (cz_any, cz_ref), (cx_any, cx_ref),
                (cy_any, cy_ref), (right_any, right_ref),
            ]
        )
    ]
    for load in loads:
        load.start()
    for load in loads[1:]:
        load.wait()

    lane = lax.broadcasted_iota(jnp.int32, (columns, cells), 1)
    row = lax.broadcasted_iota(jnp.int32, (columns, cells), 0)
    cx = cx_ref[...]
    cy, lower_z, upper_z, centre = [], [], [], []
    for d in range(depth):
        cz = cz_ref[d]
        above = pltpu.roll(cz, cells - 1, 1)
        cy.append(jnp.broadcast_to(cy_ref[d : d + 1, :], (columns, cells)))
        centre.append(2.0 * cx + 2.0 * cy[d] + cz + above)
        lower_z.append(jnp.where(lane == 0, 0.0, cz))
        upper_z.append(jnp.where(lane == cells - 1, 0.0, above))

    nothing = jnp.zeros((columns, cells), jnp.float32)
    no_edge = jnp.zeros((2 * depth, 1, cells), jnp.float32)
    no_row = jnp.zeros((1, cells), jnp.float32)
    both_rows = jnp.zeros((2, 1, cells), jnp.float32)

    @pl.when(w == 0)
    def _():
        for k in range(2):
            from_lower_half[k] = nothing
            from_lower[k] = nothing
            lower_half_rim[k] = both_rows
        lower_field_rim[...] = both_rows

    @pl.when(w == sections - 1)
    def _():
        for k in range(2):
            from_upper[k] = nothing
        upper_field_rim[...] = both_rows

    for side, last in ((0, 0), (1, strips - 1)):

        @pl.when(p == last)
        def _():
            for k in range(2):
                half_halo[k, side] = no_edge
                field_halo[k, side] = no_edge
                lower_half_rim[k, side] = no_row
            lower_field_rim[side] = no_row
            upper_field_rim[side] = no_row
            still_rim[side] = jnp.zeros(still_rim.shape[1:], jnp.float32)
            block_rim[side] = jnp.zeros(block_rim.shape[1:], jnp.float32)

    for side, c in ((0, 0), (1, columns - 1)):
        for d in range(depth):
            still_edge[side, d] = right_ref[d, c : c + 1, :]
            still_edge[side, depth + d] = cz_ref[d, c : c + 1, :]
        still_edge[side, 2 * depth] = cx[c : c + 1, :]

    loads[0].wait()
    for d in range(depth):
        for c in range(columns):
            weights[d, pl.ds(c, cells, stride=columns), :] = block[d, c].T

    def apply_block(d, v):
        parts = [None] * 4
        for j in range(cells):
            term = weights[d, pl.ds(j * columns, columns), :] * jnp.broadcast_to(
                v[:, j : j + 1], (columns, cells)
            )
            parts[j % 4] = term if parts[j % 4] is None else parts[j % 4] + term
        return relax * ((parts[0] + parts[1]) + (parts[2] + parts[3]))

    def column_part(d, v):
        return (
            centre[d] * v
            - lower_z[d] * pltpu.roll(v, 1, 1)
            - upper_z[d] * pltpu.roll(v, cells - 1, 1)
        )

    rim_lane = lax.broadcasted_iota(jnp.int32, (2, cells), 1)

    def two(low, high):
        pair_row = lax.broadcasted_iota(jnp.int32, (2, cells), 0)
        return jnp.where(
            pair_row == 0, jnp.broadcast_to(low, (2, cells)), jnp.broadcast_to(high, (2, cells))
        )

    def edges_of(v):
        return two(v[:1], v[columns - 1 :])

    def apply_rim(d, v):
        parts = [None] * 4
        for j in range(cells):
            term = weights_rim[d, pl.ds(8 * j, 2), :] * jnp.broadcast_to(
                v[:, j : j + 1], (2, cells)
            )
            parts[j % 4] = term if parts[j % 4] is None else parts[j % 4] + term
        return relax * ((parts[0] + parts[1]) + (parts[2] + parts[3]))

    def cx_rim():
        return two(still_rim[0, 2 * depth], still_rim[1, 2 * depth])

    def right_rim(d):
        return two(still_rim[0, d], still_rim[1, d])

    def column_rim(d, v):
        cz = two(still_rim[0, depth + d], still_rim[1, depth + d])
        above = pltpu.roll(cz, cells - 1, 1)
        middle = 2.0 * cx_rim() + 2.0 * cy[d][:2] + cz + above
        return (
            middle * v
            - jnp.where(rim_lane == 0, 0.0, cz) * pltpu.roll(v, 1, 1)
            - jnp.where(rim_lane == cells - 1, 0.0, above) * pltpu.roll(v, cells - 1, 1)
        )

    def still_copies(side):
        target = (w, p + (2 * side - 1))
        return [
            pltpu.make_async_remote_copy(
                src_ref=source, dst_ref=aim, send_sem=send_still.at[2 * side + i],
                recv_sem=recv_still.at[2 * side + i], device_id=target, device_id_type=MESH,
            )
            for i, (source, aim) in enumerate(
                [
                    (still_edge.at[side], still_rim.at[1 - side]),
                    (block.at[:, 0 if side == 0 else columns - 1], block_rim.at[1 - side]),
                ]
            )
        ]

    def on_sides(action, arriving):
        for side in range(2):
            ok = (p > 0) if (side == 0) != arriving else (p < strips - 1)

            @pl.when(ok)
            def _():
                action(side)

    def start_still():
        on_sides(lambda side: [c.start() for c in still_copies(side)], False)

    def rim_ready():
        on_sides(lambda side: [c.wait_recv() for c in still_copies(side)], True)
        for side in range(2):
            for d in range(depth):
                weights_rim[d, pl.ds(side, cells, stride=8), :] = block_rim[side, d].T

    def d_copy(source, target, side, slot, step):
        return pltpu.make_async_remote_copy(
            src_ref=source, dst_ref=target.at[1 - side],
            send_sem=send_d.at[slot + side], recv_sem=recv_d.at[slot + side],
            device_id=(w + step, p + (2 * side - 1)), device_id_type=MESH,
        )

    def up_half_rim(k):
        return lambda side: d_copy(
            half_edge.at[k, side, depth - 1], lower_half_rim.at[k], side, 2 * k, 1
        )

    def down_field_rim(side):
        return d_copy(field_edge.at[0, side, 0], upper_field_rim, side, 4, -1)

    def up_field_rim(side):
        return d_copy(field_edge.at[0, side, depth - 1], lower_field_rim, side, 6, 1)

    def along_y(v, low, high):
        below = jnp.where(row == 0, low, pltpu.roll(v, 1, 0))
        above = jnp.where(row == columns - 1, high, pltpu.roll(v, columns - 1, 0))
        return below + above

    def x_copy(source, target, slot, step):
        return pltpu.make_async_remote_copy(
            src_ref=source, dst_ref=target, send_sem=send_x.at[slot], recv_sem=recv_x.at[slot],
            device_id=(w + step, p), device_id_type=MESH,
        )

    def y_copy(edges, halo, k, side, slot):
        return pltpu.make_async_remote_copy(
            src_ref=edges.at[k, side], dst_ref=halo.at[k, 1 - side],
            send_sem=send_y.at[slot + side], recv_sem=recv_y.at[slot + side],
            device_id=(w, p + (2 * side - 1)), device_id_type=MESH,
        )

    def store_edges(planes, edges, k):
        for d in range(depth):
            edges[k, 0, d] = planes[d][:1]
            edges[k, 1, d] = planes[d][columns - 1 :]
            edges[k, 0, depth + d] = planes[d][1:2]
            edges[k, 1, depth + d] = planes[d][columns - 2 : columns - 1]

    def send_edges(edges, halo, k, slot):
        @pl.when(p > 0)
        def _():
            y_copy(edges, halo, k, 0, slot).start()

        @pl.when(p < strips - 1)
        def _():
            y_copy(edges, halo, k, 1, slot).start()

    def wait_edges(edges, halo, k, slot):
        @pl.when(p > 0)
        def _():
            y_copy(edges, halo, k, 1, slot).wait_recv()

        @pl.when(p < strips - 1)
        def _():
            y_copy(edges, halo, k, 0, slot).wait_recv()

    def wait_sent(edges, halo, k, slot):
        @pl.when(p > 0)
        def _():
            y_copy(edges, halo, k, 0, slot).wait_send()

        @pl.when(p < strips - 1)
        def _():
            y_copy(edges, halo, k, 1, slot).wait_send()

    def precondition(source, source_rim, k, meanwhile):
        slot = 3 * k
        edge_slot = 4 * k
        ahead = RIM_FIRST or k == 1
        up_half = x_copy(half.at[k, depth - 1], from_lower_half.at[k], slot, 1)
        down_field = x_copy(field.at[k, 0], from_upper.at[k], slot + 1, -1)
        up_field = x_copy(field.at[k, depth - 1], from_lower.at[k], slot + 2, 1)

        @pl.when(w > 0)
        def _():
            if k == 0:
                pl.semaphore_wait(barrier, greeted)
                start_still()
            up_half.wait_recv()

        lower = [from_lower_half[k]]
        h = []
        for d in range(depth):
            h.append(apply_block(d, source[d] + cx * lower[d]))
            lower.append(h[d])
            half[k, d] = h[d]

        if k == 0:

            @pl.when(w == 0)
            def _():
                pl.semaphore_wait(barrier, greeted)

        @pl.when(w < sections - 1)
        def _():
            up_half.start()

        store_edges(h, half_edge, k)
        if ahead:

            @pl.when(w < sections - 1)
            def _():
                on_sides(lambda side: up_half_rim(k)(side).start(), False)

        send_edges(half_edge, half_halo, k, edge_slot)
        if k == 0:

            @pl.when(w == 0)
            def _():
                start_still()

        meanwhile()
        partial = [source[d] - (column_part(d, h[d]) - cx * lower[d]) for d in range(depth)]
        if k == 0:
            rim_ready()

        def take_halo():
            wait_edges(half_edge, half_halo, k, edge_slot)
            for d in range(depth):
                half_rim[d] = two(half_halo[k, 0, d], half_halo[k, 1, d])

        if ahead:
            pl.when(w == 0)(take_halo)

            @pl.when(w > 0)
            def _():
                on_sides(lambda side: up_half_rim(k)(side).wait_recv(), True)
                previous = two(lower_half_rim[k, 0], lower_half_rim[k, 1])
                for d in range(depth):
                    previous = apply_rim(d, source_rim(d) + cx_rim() * previous)
                    half_rim[d] = previous

        else:
            take_halo()

        rest = [
            partial[d] + cy[d] * along_y(h[d], half_rim[d, 0:1], half_rim[d, 1:2])
            for d in range(depth)
        ]

        @pl.when(w < sections - 1)
        def _():
            down_field.wait_recv()

        upper = from_upper[k]
        z = [None] * depth
        above = [None] * depth
        previous = upper
        for d in reversed(range(depth)):
            above[d] = previous
            z[d] = h[d] + apply_block(d, rest[d] + cx * previous)
            previous = z[d]
            field[k, d] = z[d]

        @pl.when(w > 0)
        def _():
            down_field.start()

        @pl.when(w < sections - 1)
        def _():
            up_field.start()

        store_edges(z, field_edge, k)
        if k == 0:

            @pl.when(w > 0)
            def _():
                on_sides(lambda side: down_field_rim(side).start(), False)

            @pl.when(w < sections - 1)
            def _():
                on_sides(lambda side: up_field_rim(side).start(), False)

        send_edges(field_edge, field_halo, k, edge_slot + 2)
        if k == 0:

            @pl.when(w < sections - 1)
            def _():
                on_sides(lambda side: down_field_rim(side).wait_recv(), True)

            @pl.when(w == 0)
            def _():
                previous = two(upper_field_rim[0], upper_field_rim[1])
                for d in reversed(range(depth)):
                    v = half_rim[d]
                    far = two(half_halo[0, 0, depth + d], half_halo[0, 1, depth + d])
                    left = right_rim(d) - column_rim(d, v)
                    left = left + cy[d][:2] * (far + edges_of(h[d]))
                    if d > 0:
                        left = left + cx_rim() * half_rim[d - 1]
                    previous = v + apply_rim(d, left + cx_rim() * previous)
                    field_rim[d] = previous

        return z, above, [column_part(d, z[d]) for d in range(depth)]

    def operate(k, z, above, partial):
        edge_slot = 4 * k

        def take_halo():
            wait_edges(field_edge, field_halo, k, edge_slot + 2)
            for d in range(depth):
                field_rim[d] = two(field_halo[k, 0, d], field_halo[k, 1, d])

        if k == 0:
            pl.when(w > 0)(take_halo)
        else:
            take_halo()

        @pl.when(w > 0)
        def _():
            x_copy(field.at[k, depth - 1], from_lower.at[k], 3 * k + 2, 1).wait_recv()

        below = from_lower[k]
        image = []
        for d in range(depth):
            image.append(
                partial[d]
                - cx * (below + above[d])
                - cy[d] * along_y(z[d], field_rim[d, 0:1], field_rim[d, 1:2])
            )
            below = z[d]
        return image

    def image_rim(z):
        def at(d):
            if d == 0:
                on_sides(lambda side: up_field_rim(side).wait_recv(), True)
            low = two(lower_field_rim[0], lower_field_rim[1]) if d == 0 else field_rim[d - 1]
            high = (
                two(upper_field_rim[0], upper_field_rim[1])
                if d == depth - 1
                else field_rim[d + 1]
            )
            far = two(field_halo[0, 0, depth + d], field_halo[0, 1, depth + d])
            return (
                column_rim(d, field_rim[d])
                - cx_rim() * (low + high)
                - cy[d][:2] * (far + edges_of(z[d]))
            )

        return at

    def finish(k):
        slot = 3 * k
        edge_slot = 4 * k

        @pl.when(w < sections - 1)
        def _():
            x_copy(half.at[k, depth - 1], from_lower_half.at[k], slot, 1).wait_send()
            x_copy(field.at[k, depth - 1], from_lower.at[k], slot + 2, 1).wait_send()

        @pl.when(w > 0)
        def _():
            x_copy(field.at[k, 0], from_upper.at[k], slot + 1, -1).wait_send()

        if RIM_FIRST or k == 1:

            @pl.when(w > 0)
            def _():
                wait_edges(half_edge, half_halo, k, edge_slot)

            @pl.when(w < sections - 1)
            def _():
                on_sides(lambda side: up_half_rim(k)(side).wait_send(), False)

        if k == 0:
            on_sides(lambda side: [c.wait_send() for c in still_copies(side)], False)

            @pl.when(w == 0)
            def _():
                wait_edges(field_edge, field_halo, 0, 2)

            @pl.when(w > 0)
            def _():
                on_sides(lambda side: down_field_rim(side).wait_send(), False)

            @pl.when(w < sections - 1)
            def _():
                on_sides(lambda side: up_field_rim(side).wait_send(), False)

        wait_sent(half_edge, half_halo, k, edge_slot)
        wait_sent(field_edge, field_halo, k, edge_slot + 2)

    def inner(a, b):
        total = a[0] * b[0]
        for d in range(1, depth):
            total = total + a[d] * b[d]
        return jnp.sum(jnp.sum(total, axis=0, keepdims=True), axis=1, keepdims=True)

    spot = lax.broadcasted_iota(jnp.int32, (1, cells), 1)
    rows = 1 + 2 * depth
    right = [right_ref[d] for d in range(depth)]
    z, above, partial = precondition(right, right_rim, 0, lambda: None)
    q = operate(0, z, above, partial)

    def early():
        sums[0, 0] = jnp.where(
            spot == 0, inner(z, right), jnp.where(spot == 1, inner(z, q), 0.0)
        )

    y, above, partial = precondition(q, image_rim(z), 1, early)
    faced = []
    for d in range(depth):
        next_column = jnp.where(row == columns - 1, 0.0, pltpu.roll(y[d], columns - 1, 0))
        faced.append(partial[d] - 2.0 * (cx * above[d] + cy[d] * next_column))
        sums[0, 1 + 2 * d] = y[d][:1]
        sums[0, 2 + 2 * d] = cy[d][:1] * y[d][columns - 1 :]
    packed = sums[0, 0]
    for i, (a, b) in enumerate([(y, q), (y, right), (y, faced)]):
        packed = jnp.where(spot == 2 + i, inner(a, b), packed)

    base = 0
    for stage, (count, me, where) in enumerate(groups):
        width = rows if stage == 0 else 1
        sums[stage, 0] = packed

        def send(offset):
            return pltpu.make_async_remote_copy(
                src_ref=sums.at[stage, pl.ds(0, width)],
                dst_ref=gathered.at[base + me, pl.ds(0, width)],
                send_sem=send_sum.at[base + offset], recv_sem=recv_sum.at[base + me],
                device_id=where((me + offset) % count), device_id_type=MESH,
            )

        def arrival(sender):
            return pltpu.make_async_remote_copy(
                src_ref=sums.at[stage, pl.ds(0, width)],
                dst_ref=gathered.at[base + sender, pl.ds(0, width)],
                send_sem=send_sum.at[base], recv_sem=recv_sum.at[base + sender],
                device_id=where(sender), device_id_type=MESH,
            )

        for offset in range(1, count):
            send(offset).start()
        for i in range(width):
            gathered[base + me, i] = sums[stage, i]
        if stage == 0:
            u = operate(1, y, above, partial)
            finish(0)
            finish(1)
        for offset in range(1, count):
            arrival((me + offset) % count).wait_recv()

        def tree(parts):
            while len(parts) > 1:
                parts = [
                    parts[i] + parts[i + 1] if i + 1 < len(parts) else parts[i]
                    for i in range(0, len(parts), 2)
                ]
            return parts[0]

        packed = tree([gathered[base + i, 0] for i in range(count)])
        faces = [
            gathered[base + i, 2 + 2 * d] * gathered[base + i + 1, 1 + 2 * d]
            for i in range(count)
            if stage == 0 and i % strips != strips - 1
            for d in range(depth)
        ]
        if faces:
            across = jnp.sum(tree(faces), axis=1, keepdims=True)
            packed = jnp.where(spot == 4, packed - 2.0 * across, packed)
        for offset in range(1, count):
            send(offset).wait_send()
        base += count

    zr, zq, yq, yr, yu = [
        jnp.broadcast_to(packed[:, i : i + 1], (1, cells)) for i in range(5)
    ]
    first_step = zr / zq
    keep = 1.0 - (zq - first_step * yq) / zq
    projection = keep * (zr - first_step * zq) - first_step * (yr - first_step * yq)
    curvature = (
        keep * keep * zq - keep * 2.0 * first_step * yq + first_step * first_step * yu
    )
    step = projection / curvature
    of_z = first_step + step * keep
    of_y = step * first_step
    for d in range(depth):
        solution_ref[d] = of_z * z[d] - of_y * y[d]
        residual_ref[d] = right[d] - of_z * q[d] + of_y * u[d]


def solution(mesh):
    sections = mesh.shape["wave"]
    strips = mesh.shape["plane"]

    def on_device(right_side, coupling_x, coupling_y, coupling_z, inverse):
        depth, columns, cells = right_side.shape
        devices = sections * strips
        slots = devices if devices <= DIRECT else sections + strips
        vmem = pl.BlockSpec(memory_space=pltpu.VMEM)
        plane = (columns, cells)
        out = pltpu.VMEM(right_side.shape, jnp.float32)
        rows = 1 + 2 * depth
        return pl.pallas_call(
            functools.partial(kernel, sections, strips),
            out_shape=(out, out),
            in_specs=[pl.BlockSpec(memory_space=pl.ANY)] * 5,
            out_specs=(vmem, vmem),
            scratch_shapes=[
                pltpu.VMEM(right_side.shape, jnp.float32),
                pltpu.VMEM(coupling_x.shape, jnp.float32),
                pltpu.VMEM(coupling_y.shape, jnp.float32),
                pltpu.VMEM(coupling_z.shape, jnp.float32),
                pltpu.VMEM(inverse.shape, jnp.float32),
                pltpu.VMEM((depth, cells * columns, cells), jnp.float32),
                pltpu.VMEM((2, depth) + plane, jnp.float32),
                pltpu.VMEM((2, depth) + plane, jnp.float32),
                pltpu.VMEM((2, 2, 2 * depth, 1, cells), jnp.float32),
                pltpu.VMEM((2, 2, 2 * depth, 1, cells), jnp.float32),
                pltpu.VMEM((2,) + plane, jnp.float32),
                pltpu.VMEM((2,) + plane, jnp.float32),
                pltpu.VMEM((2,) + plane, jnp.float32),
                pltpu.VMEM((2, 2, 2 * depth, 1, cells), jnp.float32),
                pltpu.VMEM((2, 2, 2 * depth, 1, cells), jnp.float32),
                pltpu.VMEM((2, 2 * depth + 1, 1, cells), jnp.float32),
                pltpu.VMEM((2, 2 * depth + 1, 1, cells), jnp.float32),
                pltpu.VMEM((2, depth, cells, cells), jnp.float32),
                pltpu.VMEM((depth, 8 * cells, cells), jnp.float32),
                pltpu.VMEM((depth, 2, cells), jnp.float32),
                pltpu.VMEM((depth, 2, cells), jnp.float32),
                pltpu.VMEM((2, 2, 1, cells), jnp.float32),
                pltpu.VMEM((2, 1, cells), jnp.float32),
                pltpu.VMEM((2, 1, cells), jnp.float32),
                pltpu.VMEM((2, rows, 1, cells), jnp.float32),
                pltpu.VMEM((slots, rows, 1, cells), jnp.float32),
                pltpu.SemaphoreType.DMA((5,)),
                pltpu.SemaphoreType.DMA((6,)),
                pltpu.SemaphoreType.DMA((6,)),
                pltpu.SemaphoreType.DMA((8,)),
                pltpu.SemaphoreType.DMA((8,)),
                pltpu.SemaphoreType.DMA((8,)),
                pltpu.SemaphoreType.DMA((8,)),
                pltpu.SemaphoreType.DMA((4,)),
                pltpu.SemaphoreType.DMA((4,)),
                pltpu.SemaphoreType.DMA((slots,)),
                pltpu.SemaphoreType.DMA((slots,)),
            ],
            compiler_params=pltpu.CompilerParams(collective_id=0, has_side_effects=True),
        )(right_side, coupling_x, coupling_y, coupling_z, inverse)

    placed = (
        P("wave", "plane", None),
        P("plane", None),
        P("wave", None),
        P("wave", "plane", None),
        P("wave", "plane", None, None),
    )
    return jax.shard_map(
        on_device,
        mesh=mesh,
        in_specs=placed,
        out_specs=(P("wave", "plane", None), P("wave", "plane", None)),
        check_vma=False,
    )
```

```python
import functools

import jax
import jax.numpy as jnp
from jax import lax
from jax.experimental import pallas as pl
from jax.experimental.pallas import tpu as pltpu
from jax.sharding import PartitionSpec as P

relax = 1.5
MESH = pl.DeviceIdType.MESH
DIRECT = 64
RIM_FIRST = True


def kernel(
    sections, strips,
    right_any, cx_any, cy_any, cz_any, inverse_any,
    solution_ref, residual_ref,
    right_ref, cx_ref, cy_ref, cz_ref, block, weights, half, field, half_edge, field_edge,
    from_lower_half, from_upper, from_lower, half_halo, field_halo,
    still_edge, still_rim, block_rim, weights_rim, half_rim, field_rim,
    lower_half_rim, upper_field_rim, lower_field_rim,
    sums, gathered,
    load_sem, send_x, recv_x, send_y, recv_y, send_d, recv_d, send_still, recv_still, send_sum, recv_sum,
):
    depth, columns, cells = right_ref.shape
    w = lax.axis_index("wave")
    p = lax.axis_index("plane")
    devices = sections * strips

    barrier = pltpu.get_barrier_semaphore()
    single = devices <= DIRECT
    if single:
        groups = [(devices, w * strips + p, lambda t: (t // strips, t % strips))]
    else:
        groups = [(strips, p, lambda t: (w, t)), (sections, w, lambda t: (t, p))]
    greeted = 0
    for count, me, where in groups:
        for offset in range(1, count):
            pl.semaphore_signal(
                barrier, inc=1, device_id=where((me + offset) % count), device_id_type=MESH
            )
        greeted += count - 1
    if not single:
        for a in (-1, 1):
            for b in (-1, 1):
                near = (
                    (w + a >= 0) & (w + a < sections) & (p + b >= 0) & (p + b < strips)
                )
                greeted = greeted + near.astype(jnp.int32)

                @pl.when(near)
                def _():
                    pl.semaphore_signal(
                        barrier, inc=1, device_id=(w + a, p + b), device_id_type=MESH
                    )

    loads = [
        pltpu.make_async_copy(source, target, load_sem.at[i])
        for i, (source, target) in enumerate(
            [
                (inverse_any, block), (cz_any, cz_ref), (cx_any, cx_ref),
                (cy_any, cy_ref), (right_any, right_ref),
            ]
        )
    ]
    for load in loads:
        load.start()
    for load in loads[1:]:
        load.wait()

    lane = lax.broadcasted_iota(jnp.int32, (columns, cells), 1)
    row = lax.broadcasted_iota(jnp.int32, (columns, cells), 0)
    cx = cx_ref[...]
    cy, lower_z, upper_z, centre = [], [], [], []
    for d in range(depth):
        cz = cz_ref[d]
        above = pltpu.roll(cz, cells - 1, 1)
        cy.append(jnp.broadcast_to(cy_ref[d : d + 1, :], (columns, cells)))
        centre.append(2.0 * cx + 2.0 * cy[d] + cz + above)
        lower_z.append(jnp.where(lane == 0, 0.0, cz))
        upper_z.append(jnp.where(lane == cells - 1, 0.0, above))

    nothing = jnp.zeros((columns, cells), jnp.float32)
    no_edge = jnp.zeros((2 * depth, 1, cells), jnp.float32)
    no_row = jnp.zeros((1, cells), jnp.float32)
    both_rows = jnp.zeros((2, 1, cells), jnp.float32)

    @pl.when(w == 0)
    def _():
        for k in range(2):
            from_lower_half[k] = nothing
            from_lower[k] = nothing
            lower_half_rim[k] = both_rows
        lower_field_rim[...] = both_rows

    @pl.when(w == sections - 1)
    def _():
        for k in range(2):
            from_upper[k] = nothing
        upper_field_rim[...] = both_rows

    for side, last in ((0, 0), (1, strips - 1)):

        @pl.when(p == last)
        def _():
            for k in range(2):
                half_halo[k, side] = no_edge
                field_halo[k, side] = no_edge
                lower_half_rim[k, side] = no_row
            lower_field_rim[side] = no_row
            upper_field_rim[side] = no_row
            still_rim[side] = jnp.zeros(still_rim.shape[1:], jnp.float32)
            block_rim[side] = jnp.zeros(block_rim.shape[1:], jnp.float32)

    for side, c in ((0, 0), (1, columns - 1)):
        for d in range(depth):
            still_edge[side, d] = right_ref[d, c : c + 1, :]
            still_edge[side, depth + d] = cz_ref[d, c : c + 1, :]
        still_edge[side, 2 * depth] = cx[c : c + 1, :]

    loads[0].wait()
    for d in range(depth):
        for c in range(columns):
            weights[d, pl.ds(c, cells, stride=columns), :] = block[d, c].T

    def apply_block(d, v):
        parts = [None] * 4
        for j in range(cells):
            term = weights[d, pl.ds(j * columns, columns), :] * jnp.broadcast_to(
                v[:, j : j + 1], (columns, cells)
            )
            parts[j % 4] = term if parts[j % 4] is None else parts[j % 4] + term
        return relax * ((parts[0] + parts[1]) + (parts[2] + parts[3]))

    def column_part(d, v):
        return (
            centre[d] * v
            - lower_z[d] * pltpu.roll(v, 1, 1)
            - upper_z[d] * pltpu.roll(v, cells - 1, 1)
        )

    rim_lane = lax.broadcasted_iota(jnp.int32, (2, cells), 1)

    def two(low, high):
        pair_row = lax.broadcasted_iota(jnp.int32, (2, cells), 0)
        return jnp.where(
            pair_row == 0, jnp.broadcast_to(low, (2, cells)), jnp.broadcast_to(high, (2, cells))
        )

    def edges_of(v):
        return two(v[:1], v[columns - 1 :])

    def apply_rim(d, v):
        parts = [None] * 4
        for j in range(cells):
            term = weights_rim[d, pl.ds(8 * j, 2), :] * jnp.broadcast_to(
                v[:, j : j + 1], (2, cells)
            )
            parts[j % 4] = term if parts[j % 4] is None else parts[j % 4] + term
        return relax * ((parts[0] + parts[1]) + (parts[2] + parts[3]))

    def cx_rim():
        return two(still_rim[0, 2 * depth], still_rim[1, 2 * depth])

    def right_rim(d):
        return two(still_rim[0, d], still_rim[1, d])

    def column_rim(d, v):
        cz = two(still_rim[0, depth + d], still_rim[1, depth + d])
        above = pltpu.roll(cz, cells - 1, 1)
        middle = 2.0 * cx_rim() + 2.0 * cy[d][:2] + cz + above
        return (
            middle * v
            - jnp.where(rim_lane == 0, 0.0, cz) * pltpu.roll(v, 1, 1)
            - jnp.where(rim_lane == cells - 1, 0.0, above) * pltpu.roll(v, cells - 1, 1)
        )

    def still_copies(side):
        target = (w, p + (2 * side - 1))
        return [
            pltpu.make_async_remote_copy(
                src_ref=source, dst_ref=aim, send_sem=send_still.at[2 * side + i],
                recv_sem=recv_still.at[2 * side + i], device_id=target, device_id_type=MESH,
            )
            for i, (source, aim) in enumerate(
                [
                    (still_edge.at[side], still_rim.at[1 - side]),
                    (block.at[:, 0 if side == 0 else columns - 1], block_rim.at[1 - side]),
                ]
            )
        ]

    def on_sides(action, arriving):
        for side in range(2):
            ok = (p > 0) if (side == 0) != arriving else (p < strips - 1)

            @pl.when(ok)
            def _():
                action(side)

    def start_still():
        on_sides(lambda side: [c.start() for c in still_copies(side)], False)

    def rim_ready():
        on_sides(lambda side: [c.wait_recv() for c in still_copies(side)], True)
        for side in range(2):
            for d in range(depth):
                weights_rim[d, pl.ds(side, cells, stride=8), :] = block_rim[side, d].T

    def d_copy(source, target, side, slot, step):
        return pltpu.make_async_remote_copy(
            src_ref=source, dst_ref=target.at[1 - side],
            send_sem=send_d.at[slot + side], recv_sem=recv_d.at[slot + side],
            device_id=(w + step, p + (2 * side - 1)), device_id_type=MESH,
        )

    def up_half_rim(k):
        return lambda side: d_copy(
            half_edge.at[k, side, depth - 1], lower_half_rim.at[k], side, 2 * k, 1
        )

    def down_field_rim(side):
        return d_copy(field_edge.at[0, side, 0], upper_field_rim, side, 4, -1)

    def up_field_rim(side):
        return d_copy(field_edge.at[0, side, depth - 1], lower_field_rim, side, 6, 1)

    def along_y(v, low, high):
        below = jnp.where(row == 0, low, pltpu.roll(v, 1, 0))
        above = jnp.where(row == columns - 1, high, pltpu.roll(v, columns - 1, 0))
        return below + above

    def x_copy(source, target, slot, step):
        return pltpu.make_async_remote_copy(
            src_ref=source, dst_ref=target, send_sem=send_x.at[slot], recv_sem=recv_x.at[slot],
            device_id=(w + step, p), device_id_type=MESH,
        )

    def y_copy(edges, halo, k, side, slot):
        return pltpu.make_async_remote_copy(
            src_ref=edges.at[k, side], dst_ref=halo.at[k, 1 - side],
            send_sem=send_y.at[slot + side], recv_sem=recv_y.at[slot + side],
            device_id=(w, p + (2 * side - 1)), device_id_type=MESH,
        )

    def store_edges(planes, edges, k):
        for d in range(depth):
            edges[k, 0, d] = planes[d][:1]
            edges[k, 1, d] = planes[d][columns - 1 :]
            edges[k, 0, depth + d] = planes[d][1:2]
            edges[k, 1, depth + d] = planes[d][columns - 2 : columns - 1]

    def send_edges(edges, halo, k, slot):
        @pl.when(p > 0)
        def _():
            y_copy(edges, halo, k, 0, slot).start()

        @pl.when(p < strips - 1)
        def _():
            y_copy(edges, halo, k, 1, slot).start()

    def wait_edges(edges, halo, k, slot):
        @pl.when(p > 0)
        def _():
            y_copy(edges, halo, k, 1, slot).wait_recv()

        @pl.when(p < strips - 1)
        def _():
            y_copy(edges, halo, k, 0, slot).wait_recv()

    def wait_sent(edges, halo, k, slot):
        @pl.when(p > 0)
        def _():
            y_copy(edges, halo, k, 0, slot).wait_send()

        @pl.when(p < strips - 1)
        def _():
            y_copy(edges, halo, k, 1, slot).wait_send()

    def precondition(source, source_rim, k, meanwhile):
        slot = 3 * k
        edge_slot = 4 * k
        ahead = RIM_FIRST or k == 1
        up_half = x_copy(half.at[k, depth - 1], from_lower_half.at[k], slot, 1)
        down_field = x_copy(field.at[k, 0], from_upper.at[k], slot + 1, -1)
        up_field = x_copy(field.at[k, depth - 1], from_lower.at[k], slot + 2, 1)

        @pl.when(w > 0)
        def _():
            if k == 0:
                pl.semaphore_wait(barrier, greeted)
                start_still()
            up_half.wait_recv()

        lower = [from_lower_half[k]]
        h = []
        for d in range(depth):
            h.append(apply_block(d, source[d] + cx * lower[d]))
            lower.append(h[d])
            half[k, d] = h[d]

        if k == 0:

            @pl.when(w == 0)
            def _():
                pl.semaphore_wait(barrier, greeted)

        @pl.when(w < sections - 1)
        def _():
            up_half.start()

        store_edges(h, half_edge, k)
        if ahead:

            @pl.when(w < sections - 1)
            def _():
                on_sides(lambda side: up_half_rim(k)(side).start(), False)

        send_edges(half_edge, half_halo, k, edge_slot)
        if k == 0:

            @pl.when(w == 0)
            def _():
                start_still()

        meanwhile()
        partial = [source[d] - (column_part(d, h[d]) - cx * lower[d]) for d in range(depth)]
        if k == 0:
            rim_ready()

        def take_halo():
            wait_edges(half_edge, half_halo, k, edge_slot)
            for d in range(depth):
                half_rim[d] = two(half_halo[k, 0, d], half_halo[k, 1, d])

        if ahead:
            pl.when(w == 0)(take_halo)

            @pl.when(w > 0)
            def _():
                on_sides(lambda side: up_half_rim(k)(side).wait_recv(), True)
                previous = two(lower_half_rim[k, 0], lower_half_rim[k, 1])
                for d in range(depth):
                    previous = apply_rim(d, source_rim(d) + cx_rim() * previous)
                    half_rim[d] = previous

        else:
            take_halo()

        rest = [
            partial[d] + cy[d] * along_y(h[d], half_rim[d, 0:1], half_rim[d, 1:2])
            for d in range(depth)
        ]

        @pl.when(w < sections - 1)
        def _():
            down_field.wait_recv()

        upper = from_upper[k]
        z = [None] * depth
        above = [None] * depth
        previous = upper
        for d in reversed(range(depth)):
            above[d] = previous
            z[d] = h[d] + apply_block(d, rest[d] + cx * previous)
            previous = z[d]
            field[k, d] = z[d]

        @pl.when(w > 0)
        def _():
            down_field.start()

        @pl.when(w < sections - 1)
        def _():
            up_field.start()

        store_edges(z, field_edge, k)
        if k == 0:

            @pl.when(w > 0)
            def _():
                on_sides(lambda side: down_field_rim(side).start(), False)

            @pl.when(w < sections - 1)
            def _():
                on_sides(lambda side: up_field_rim(side).start(), False)

        send_edges(field_edge, field_halo, k, edge_slot + 2)
        if k == 0:

            @pl.when(w < sections - 1)
            def _():
                on_sides(lambda side: down_field_rim(side).wait_recv(), True)

            @pl.when(w == 0)
            def _():
                previous = two(upper_field_rim[0], upper_field_rim[1])
                for d in reversed(range(depth)):
                    v = half_rim[d]
                    far = two(half_halo[0, 0, depth + d], half_halo[0, 1, depth + d])
                    left = right_rim(d) - column_rim(d, v)
                    left = left + cy[d][:2] * (far + edges_of(h[d]))
                    if d > 0:
                        left = left + cx_rim() * half_rim[d - 1]
                    previous = v + apply_rim(d, left + cx_rim() * previous)
                    field_rim[d] = previous

        return z, above, [column_part(d, z[d]) for d in range(depth)]

    def operate(k, z, above, partial):
        edge_slot = 4 * k

        def take_halo():
            wait_edges(field_edge, field_halo, k, edge_slot + 2)
            for d in range(depth):
                field_rim[d] = two(field_halo[k, 0, d], field_halo[k, 1, d])

        if k == 0:
            pl.when(w > 0)(take_halo)
        else:
            take_halo()

        @pl.when(w > 0)
        def _():
            x_copy(field.at[k, depth - 1], from_lower.at[k], 3 * k + 2, 1).wait_recv()

        below = from_lower[k]
        image = []
        for d in range(depth):
            image.append(
                partial[d]
                - cx * (below + above[d])
                - cy[d] * along_y(z[d], field_rim[d, 0:1], field_rim[d, 1:2])
            )
            below = z[d]
        return image

    def image_rim(z):
        def at(d):
            if d == 0:
                on_sides(lambda side: up_field_rim(side).wait_recv(), True)
            low = two(lower_field_rim[0], lower_field_rim[1]) if d == 0 else field_rim[d - 1]
            high = (
                two(upper_field_rim[0], upper_field_rim[1])
                if d == depth - 1
                else field_rim[d + 1]
            )
            far = two(field_halo[0, 0, depth + d], field_halo[0, 1, depth + d])
            return (
                column_rim(d, field_rim[d])
                - cx_rim() * (low + high)
                - cy[d][:2] * (far + edges_of(z[d]))
            )

        return at

    def finish(k):
        slot = 3 * k
        edge_slot = 4 * k

        @pl.when(w < sections - 1)
        def _():
            x_copy(half.at[k, depth - 1], from_lower_half.at[k], slot, 1).wait_send()
            x_copy(field.at[k, depth - 1], from_lower.at[k], slot + 2, 1).wait_send()

        @pl.when(w > 0)
        def _():
            x_copy(field.at[k, 0], from_upper.at[k], slot + 1, -1).wait_send()

        if RIM_FIRST or k == 1:

            @pl.when(w > 0)
            def _():
                wait_edges(half_edge, half_halo, k, edge_slot)

            @pl.when(w < sections - 1)
            def _():
                on_sides(lambda side: up_half_rim(k)(side).wait_send(), False)

        if k == 0:
            on_sides(lambda side: [c.wait_send() for c in still_copies(side)], False)

            @pl.when(w == 0)
            def _():
                wait_edges(field_edge, field_halo, 0, 2)

            @pl.when(w > 0)
            def _():
                on_sides(lambda side: down_field_rim(side).wait_send(), False)

            @pl.when(w < sections - 1)
            def _():
                on_sides(lambda side: up_field_rim(side).wait_send(), False)

        wait_sent(half_edge, half_halo, k, edge_slot)
        wait_sent(field_edge, field_halo, k, edge_slot + 2)

    def inner(a, b):
        total = a[0] * b[0]
        for d in range(1, depth):
            total = total + a[d] * b[d]
        return jnp.sum(jnp.sum(total, axis=0, keepdims=True), axis=1, keepdims=True)

    spot = lax.broadcasted_iota(jnp.int32, (1, cells), 1)
    rows = 1 + 2 * depth
    right = [right_ref[d] for d in range(depth)]
    z, above, partial = precondition(right, right_rim, 0, lambda: None)
    q = operate(0, z, above, partial)

    def early():
        sums[0, 0] = jnp.where(
            spot == 0, inner(z, right), jnp.where(spot == 1, inner(z, q), 0.0)
        )

    y, above, partial = precondition(q, image_rim(z), 1, early)
    faced = []
    for d in range(depth):
        next_column = jnp.where(row == columns - 1, 0.0, pltpu.roll(y[d], columns - 1, 0))
        faced.append(partial[d] - 2.0 * (cx * above[d] + cy[d] * next_column))
        sums[0, 1 + 2 * d] = y[d][:1]
        sums[0, 2 + 2 * d] = cy[d][:1] * y[d][columns - 1 :]
    packed = sums[0, 0]
    for i, (a, b) in enumerate([(y, q), (y, right), (y, faced)]):
        packed = jnp.where(spot == 2 + i, inner(a, b), packed)

    base = 0
    for stage, (count, me, where) in enumerate(groups):
        width = rows if stage == 0 else 1
        sums[stage, 0] = packed

        def send(offset):
            return pltpu.make_async_remote_copy(
                src_ref=sums.at[stage, pl.ds(0, width)],
                dst_ref=gathered.at[base + me, pl.ds(0, width)],
                send_sem=send_sum.at[base + offset], recv_sem=recv_sum.at[base + me],
                device_id=where((me + offset) % count), device_id_type=MESH,
            )

        def arrival(sender):
            return pltpu.make_async_remote_copy(
                src_ref=sums.at[stage, pl.ds(0, width)],
                dst_ref=gathered.at[base + sender, pl.ds(0, width)],
                send_sem=send_sum.at[base], recv_sem=recv_sum.at[base + sender],
                device_id=where(sender), device_id_type=MESH,
            )

        for offset in range(1, count):
            send(offset).start()
        for i in range(width):
            gathered[base + me, i] = sums[stage, i]
        if stage == 0:
            u = operate(1, y, above, partial)
            finish(0)
            finish(1)
        for offset in range(1, count):
            arrival((me + offset) % count).wait_recv()

        def tree(parts):
            while len(parts) > 1:
                parts = [
                    parts[i] + parts[i + 1] if i + 1 < len(parts) else parts[i]
                    for i in range(0, len(parts), 2)
                ]
            return parts[0]

        packed = tree([gathered[base + i, 0] for i in range(count)])
        faces = [
            gathered[base + i, 2 + 2 * d] * gathered[base + i + 1, 1 + 2 * d]
            for i in range(count)
            if stage == 0 and i % strips != strips - 1
            for d in range(depth)
        ]
        if faces:
            across = jnp.sum(tree(faces), axis=1, keepdims=True)
            packed = jnp.where(spot == 4, packed - 2.0 * across, packed)
        for offset in range(1, count):
            send(offset).wait_send()
        base += count

    zr, zq, yq, yr, yu = [
        jnp.broadcast_to(packed[:, i : i + 1], (1, cells)) for i in range(5)
    ]
    first_step = zr / zq
    keep = 1.0 - (zq - first_step * yq) / zq
    projection = keep * (zr - first_step * zq) - first_step * (yr - first_step * yq)
    curvature = (
        keep * keep * zq - keep * 2.0 * first_step * yq + first_step * first_step * yu
    )
    step = projection / curvature
    of_z = first_step + step * keep
    of_y = step * first_step
    for d in range(depth):
        solution_ref[d] = of_z * z[d] - of_y * y[d]
        residual_ref[d] = right[d] - of_z * q[d] + of_y * u[d]


def solution(mesh):
    sections = mesh.shape["wave"]
    strips = mesh.shape["plane"]

    def on_device(right_side, coupling_x, coupling_y, coupling_z, inverse):
        depth, columns, cells = right_side.shape
        devices = sections * strips
        slots = devices if devices <= DIRECT else sections + strips
        vmem = pl.BlockSpec(memory_space=pltpu.VMEM)
        plane = (columns, cells)
        out = pltpu.VMEM(right_side.shape, jnp.float32)
        rows = 1 + 2 * depth
        return pl.pallas_call(
            functools.partial(kernel, sections, strips),
            out_shape=(out, out),
            in_specs=[pl.BlockSpec(memory_space=pl.ANY)] * 5,
            out_specs=(vmem, vmem),
            scratch_shapes=[
                pltpu.VMEM(right_side.shape, jnp.float32),
                pltpu.VMEM(coupling_x.shape, jnp.float32),
                pltpu.VMEM(coupling_y.shape, jnp.float32),
                pltpu.VMEM(coupling_z.shape, jnp.float32),
                pltpu.VMEM(inverse.shape, jnp.float32),
                pltpu.VMEM((depth, cells * columns, cells), jnp.float32),
                pltpu.VMEM((2, depth) + plane, jnp.float32),
                pltpu.VMEM((2, depth) + plane, jnp.float32),
                pltpu.VMEM((2, 2, 2 * depth, 1, cells), jnp.float32),
                pltpu.VMEM((2, 2, 2 * depth, 1, cells), jnp.float32),
                pltpu.VMEM((2,) + plane, jnp.float32),
                pltpu.VMEM((2,) + plane, jnp.float32),
                pltpu.VMEM((2,) + plane, jnp.float32),
                pltpu.VMEM((2, 2, 2 * depth, 1, cells), jnp.float32),
                pltpu.VMEM((2, 2, 2 * depth, 1, cells), jnp.float32),
                pltpu.VMEM((2, 2 * depth + 1, 1, cells), jnp.float32),
                pltpu.VMEM((2, 2 * depth + 1, 1, cells), jnp.float32),
                pltpu.VMEM((2, depth, cells, cells), jnp.float32),
                pltpu.VMEM((depth, 8 * cells, cells), jnp.float32),
                pltpu.VMEM((depth, 2, cells), jnp.float32),
                pltpu.VMEM((depth, 2, cells), jnp.float32),
                pltpu.VMEM((2, 2, 1, cells), jnp.float32),
                pltpu.VMEM((2, 1, cells), jnp.float32),
                pltpu.VMEM((2, 1, cells), jnp.float32),
                pltpu.VMEM((2, rows, 1, cells), jnp.float32),
                pltpu.VMEM((slots, rows, 1, cells), jnp.float32),
                pltpu.SemaphoreType.DMA((5,)),
                pltpu.SemaphoreType.DMA((6,)),
                pltpu.SemaphoreType.DMA((6,)),
                pltpu.SemaphoreType.DMA((8,)),
                pltpu.SemaphoreType.DMA((8,)),
                pltpu.SemaphoreType.DMA((8,)),
                pltpu.SemaphoreType.DMA((8,)),
                pltpu.SemaphoreType.DMA((4,)),
                pltpu.SemaphoreType.DMA((4,)),
                pltpu.SemaphoreType.DMA((slots,)),
                pltpu.SemaphoreType.DMA((slots,)),
            ],
            compiler_params=pltpu.CompilerParams(collective_id=0, has_side_effects=True),
        )(right_side, coupling_x, coupling_y, coupling_z, inverse)

    placed = (
        P("wave", "plane", None),
        P("plane", None),
        P("wave", None),
        P("wave", "plane", None),
        P("wave", "plane", None, None),
    )
    return jax.shard_map(
        on_device,
        mesh=mesh,
        in_specs=placed,
        out_specs=(P("wave", "plane", None), P("wave", "plane", None)),
        check_vma=False,
    )
```
